32 devices in a mesh: dp: 4 (over y, x), mp: 8 (over z, core).
Axes of the slice: x: 2, y: 2, z: 4, core: 2. Of those that a mesh axis runs over, the one named last changes fastest.
Arguments:
- image: bfloat16 [4, 2048, 1280], P('dp', 'mp'), may hold values from -6 to 6
- ln_gain: float32 [1280], replicated, may hold values from 0.1 to 1.9
- fc1_weight: bfloat16 [1280, 5120], P(None, ('dp', 'mp')), may hold values from -0.15625 to 0.15625
- fc2_weight: bfloat16 [5120, 1280], P(('dp', 'mp')), may hold values from -0.078125 to 0.078125
- projector_weight: bfloat16 [1280, 8192], P(None, 'mp'), may hold values from -0.15625 to 0.15625
- kv_weight: bfloat16 [8192, 8, 2, 128], P('mp'), may hold values from -0.0625 to 0.0625
- text: bfloat16 [4, 128, 8192], P('dp'), may hold values from -480 to 480
- q_weight: bfloat16 [8192, 8192], P(None, 'mp'), may hold values from -0.0625 to 0.0625
- o_weight: bfloat16 [8192, 8192], P('mp'), may hold values from -0.0625 to 0.0625
- tile_count: int32 [4], P('dp'), may hold values from 1 to 4
- text_start: int32 [4], P('dp'), may hold values from 0 to 63
Outputs:
- attended: bfloat16 [4, 128, 8192], P('dp', 'mp')
The draws below stay inside these ranges and needn't reach their ends.
All inputs are finite; a program needn't handle non-finite values.
Results may differ from the reference program's by a relative error of at most 0.035.
Values may be sent and summed in bfloat16 or wider, within the bound.
A program may use at most 128 MiB of HBM per device.

```python
import jax
import jax.numpy as jnp
from jax import lax

D_VIS = 1280
VIS_FF = 5120
HEADS = 64
KV_HEADS = 8
HEAD_DIM = 128
D = 8192
MAX_TILES = 4
TILE_TOK = 512
TEXT = 128
IMG = 2048
SAMPLES = 4


def draw_text(key, part):
    base = jax.random.normal(key, (SAMPLES, TEXT, D), jnp.float32)
    return jnp.clip(base, -6.0, 6.0).astype(jnp.bfloat16)


def touch_ends(entries, stream_key, low, top_value):
    longest = entries.shape.index(max(entries.shape))
    spots = []
    for shift in (0, 1):
        where = [jax.random.randint(jax.random.fold_in(stream_key, axis), (), 0, length) for axis, length in enumerate(entries.shape)]
        where[longest] = (where[longest] + shift) % entries.shape[longest]
        spots.append(tuple(where))
    return entries.at[spots[0]].set(low).at[spots[1]].set(top_value)


def block_levels(rng, extent, shards, least, largest):
    def one(dim, blocks):
        draws = jax.random.uniform(jax.random.fold_in(jax.random.fold_in(rng, 6), dim), (blocks,), jnp.float32, least / len(shards), largest / len(shards))
        return jnp.repeat(jnp.exp(draws), extent[dim] // blocks).reshape((-1,) + (1,) * (len(extent) - dim - 1))

    level = one(*shards[0])
    for cut in shards[1:]:
        level = level * one(*cut)
    return level


def centred(stream_key, shape, scale, reach, shards=(), held_as=jnp.bfloat16):
    result = jax.random.normal(stream_key, shape, jnp.float32) * scale
    if len(shards) > 0:
        result = block_levels(stream_key, shape, shards, -0.22, 0.18) * result
    return jnp.clip(result, min=-reach, max=reach).astype(held_as)


def setup_inputs(seed: int = 0) -> dict:
    splits = jax.random.split(jax.random.key(seed), 12)
    return {
        "image": centred(splits[0], (SAMPLES, IMG, D_VIS), 1.0, 6.0, ((0, 4), (1, 8))),
        "ln_gain": jnp.clip(1.0 + 0.18 * jax.random.normal(splits[1], (D_VIS,), jnp.float32), 0.1, 1.9),
        "fc1_weight": centred(splits[2], (D_VIS, VIS_FF), D_VIS ** -0.5, 0.15625, ((1, 32),)),
        "fc2_weight": centred(splits[3], (VIS_FF, D_VIS), VIS_FF ** -0.5, 0.078125, ((0, 32),)),
        "projector_weight": centred(splits[4], (D_VIS, D), D_VIS ** -0.5, 0.15625, ((1, 8),)),
        "kv_weight": centred(splits[5], (D, KV_HEADS, 2, HEAD_DIM), D ** -0.5, 0.0625, ((0, 8),)),
        "text": draw_text(jax.random.fold_in(splits[11], 71), 0),
        "q_weight": centred(splits[7], (D, D), D ** -0.5, 0.0625, ((1, 8),)),
        "o_weight": centred(splits[8], (D, D), D ** -0.5, 0.0625, ((0, 8),)),
        "tile_count": touch_ends(jax.random.randint(splits[9], (SAMPLES,), 1, MAX_TILES + 1), jax.random.fold_in(splits[9], 1), 1, MAX_TILES).astype(jnp.int32),
        "text_start": touch_ends(jax.random.randint(splits[10], (SAMPLES,), 0, TEXT // 2), jax.random.fold_in(splits[10], 1), 0, (TEXT // 2) - 1).astype(jnp.int32),
    }


def layer_norm(values, gain):
    center = values - lax.optimization_barrier(jnp.mean(values, axis=-1, keepdims=True))
    spread = lax.optimization_barrier(jnp.mean(center * center, axis=-1, keepdims=True))
    return center * lax.rsqrt(spread + 1e-05) * gain

def reference(image, ln_gain, fc1_weight, fc2_weight, projector_weight, kv_weight, text, q_weight, o_weight, tile_count, text_start):
    group_size = HEADS // KV_HEADS
    scale = 1.0 / HEAD_DIM ** 0.5
    outputs = []
    for sample in range(SAMPLES):
        inputs = image[sample].astype(jnp.float32)
        normed = layer_norm(inputs, ln_gain).astype(jnp.bfloat16)
        hidden = jax.nn.gelu(jnp.dot(normed, fc1_weight, preferred_element_type=jnp.float32), approximate=False).astype(jnp.bfloat16)
        encoded = (inputs + jnp.dot(hidden, fc2_weight, preferred_element_type=jnp.float32)).astype(jnp.bfloat16)
        features = jnp.dot(encoded, projector_weight, preferred_element_type=jnp.float32).astype(jnp.bfloat16)
        projected = jnp.dot(features, kv_weight.reshape(D, KV_HEADS * 2 * HEAD_DIM), preferred_element_type=jnp.float32)
        projected = projected.reshape(IMG, KV_HEADS, 2, HEAD_DIM)
        keys = projected[:, :, 0, :]
        keys = keys * lax.rsqrt(lax.optimization_barrier(jnp.mean(keys * keys, axis=-1, keepdims=True)) + 1e-06)
        keys = keys.astype(jnp.bfloat16)
        values = projected[:, :, 1, :].astype(jnp.bfloat16)
        queries = jnp.dot(text[sample], q_weight, preferred_element_type=jnp.float32).astype(jnp.bfloat16)
        queries = queries.reshape(TEXT, KV_HEADS, group_size, HEAD_DIM).transpose(1, 0, 2, 3)
        tiles = jnp.arange(IMG, dtype=jnp.int32) // TILE_TOK
        valid = tiles < tile_count[sample]

        def one_group(operands):
            group_queries, group_keys, group_values = operands
            scores = jnp.einsum('tgd,kd->gtk', group_queries.astype(jnp.float32), group_keys.astype(jnp.float32)) * scale
            scores = jnp.where(valid[None, None, :], scores, -1e+30)
            top = lax.optimization_barrier(jnp.max(scores, axis=-1, keepdims=True))
            weights = jnp.exp(scores - top)
            probs = (weights / lax.optimization_barrier(jnp.sum(weights, axis=-1, keepdims=True))).astype(jnp.bfloat16)
            return jnp.einsum('gtk,kd->tgd', probs.astype(jnp.float32), group_values.astype(jnp.float32))
        attended_heads = lax.map(one_group, (queries, keys.transpose(1, 0, 2), values.transpose(1, 0, 2)))
        attended_heads = attended_heads.transpose(1, 0, 2, 3).reshape(TEXT, HEADS * HEAD_DIM)
        row_mask = (jnp.arange(TEXT, dtype=jnp.int32) >= text_start[sample]).astype(jnp.float32)
        heads_out = (attended_heads * row_mask[:, None]).astype(jnp.bfloat16)
        outputs.append(jnp.dot(heads_out, o_weight, preferred_element_type=jnp.float32).astype(jnp.bfloat16))
    return jnp.stack(outputs, axis=0)
```

```python
import functools

import jax
import jax.numpy as jnp
from jax import lax
from jax.experimental import pallas as pl
from jax.experimental.pallas import tpu as pltpu
from jax.sharding import PartitionSpec as P

HEAD_DIM = 128
TILE_TOK = 512

MESH = pl.DeviceIdType.MESH
CORES = 2


def count_copies(kind):
    name, axis = kind
    size = lax.axis_size(axis)
    if name == "chain":
        return 2 * (size // CORES - 1) + size // CORES
    if name == "partner":
        return size // CORES
    if name == "stride":
        return size // CORES - 1
    return size - 1


def exchange_kernel(kinds, *refs):
    count = len(kinds)
    sources, results = refs[:count], refs[count : 2 * count]
    local_sem = refs[2 * count]
    sends, recvs = refs[2 * count + 1 : 3 * count + 1], refs[3 * count + 1 :]
    axes = sorted({axis for _, axis in kinds})

    barrier = pltpu.get_barrier_semaphore()
    greeted = 0
    for axis in axes:
        size, me = lax.axis_size(axis), lax.axis_index(axis)
        for step in range(1, size):
            pl.semaphore_signal(
                barrier, inc=1, device_id={axis: lax.rem(me + step, size)}, device_id_type=MESH
            )
        greeted += size - 1
    pl.semaphore_wait(barrier, greeted)

    def remote(op, source, result, slot, axis, peer):
        return pltpu.make_async_remote_copy(
            src_ref=source,
            dst_ref=result,
            send_sem=sends[op].at[slot],
            recv_sem=recvs[op].at[slot],
            device_id={axis: peer},
            device_id_type=MESH,
        )

    simple, chains, locals_ = [], [], []
    for op, (name, axis) in enumerate(kinds):
        size, me = lax.axis_size(axis), lax.axis_index(axis)
        source, result = sources[op], results[op]
        core = lax.rem(me, CORES)
        spot = lax.div(me, CORES)
        partner = me + 1 - 2 * core
        if name == "gather":
            for step in range(1, size):
                copy = remote(op, source, result.at[me], step - 1, axis, lax.rem(me + step, size))
                copy.start()
                simple.append(copy)
            locals_.append(pltpu.make_async_copy(source, result.at[me], local_sem.at[op]))
        elif name == "columns":
            width = result.shape[-1]

            def column(index):
                return source.at[:, pl.ds(pl.multiple_of(index * width, width), width)]

            for step in range(1, size):
                peer = lax.rem(me + step, size)
                copy = remote(op, column(peer), result.at[me], step - 1, axis, peer)
                copy.start()
                simple.append(copy)
            locals_.append(pltpu.make_async_copy(column(me), result.at[me], local_sem.at[op]))
        elif name == "scatter":
            for step in range(1, size):
                peer = lax.rem(me + step, size)
                copy = remote(op, source.at[peer], result.at[me], step - 1, axis, peer)
                copy.start()
                simple.append(copy)
            locals_.append(pltpu.make_async_copy(source.at[me], result.at[me], local_sem.at[op]))
        elif name == "partner":
            for chip in range(size // CORES):
                copy = remote(
                    op, source.at[chip * CORES + 1 - core], result.at[chip], chip, axis, partner
                )
                copy.start()
                simple.append(copy)
        elif name == "stride":
            chips = size // CORES
            for step in range(1, chips):
                other = lax.rem(spot + step, chips)
                copy = remote(
                    op, source.at[other], result.at[spot], step - 1, axis, other * CORES + core
                )
                copy.start()
                simple.append(copy)
            locals_.append(pltpu.make_async_copy(source.at[spot], result.at[spot], local_sem.at[op]))
        else:
            chains.append((op, axis, size // CORES, me, core, spot, partner, source, result))
    for copy in locals_:
        copy.start()

    def hop(chain, source, block, slot, peer):
        op, axis, result = chain[0], chain[1], chain[-1]
        return remote(op, source, result.at[block], slot, axis, peer)

    for chain in chains:
        op, axis, chips, me, core, spot, partner, source, result = chain

        @pl.when(spot + 1 < chips)
        def _():
            hop(chain, source, me, 0, me + CORES).start()

        @pl.when(spot > 0)
        def _():
            hop(chain, source, me, chips - 1, me - CORES).start()

    for chain in chains:
        op, axis, chips, me, core, spot, partner, source, result = chain
        hop(chain, source, me, 2 * (chips - 1), partner).start()
        pltpu.make_async_copy(source, result.at[me], local_sem.at[op]).start()
    for step in range(1, max([chain[2] for chain in chains], default=0)):
        for chain in chains:
            op, axis, chips, me, core, spot, partner, source, result = chain
            for sign, base in ((1, 0), (-1, chips - 1)):
                origin_spot = spot - sign * step
                here = (origin_spot >= 0) & (origin_spot < chips)
                onward = (spot + sign >= 0) & (spot + sign < chips)
                block = me - sign * step * CORES

                @pl.when(here)
                def _():
                    held = result.at[block]
                    hop(chain, held, block, base + step - 1, me).wait_recv()

                    @pl.when(onward)
                    def _():
                        hop(chain, held, block, base + step, me + sign * CORES).start()

                    slot = 2 * (chips - 1) + lax.rem(origin_spot - spot + chips, chips)
                    hop(chain, held, block, slot, partner).start()

    for chain in chains:
        op, axis, chips, me, core, spot, partner, source, result = chain
        for step in range(chips):
            for_spot = lax.rem(spot + step, chips)
            block = for_spot * CORES + core
            theirs = for_spot * CORES + 1 - core
            slot = 2 * (chips - 1) + step
            hop(chain, result.at[block], block, slot, partner).wait_send()
            hop(chain, result.at[theirs], theirs, slot, partner).wait_recv()
        for step in range(chips - 1):
            for sign, base in ((1, 0), (-1, chips - 1)):
                origin_spot = spot - sign * step
                sent = (
                    (origin_spot >= 0)
                    & (origin_spot < chips)
                    & (spot + sign >= 0)
                    & (spot + sign < chips)
                )
                block = me - sign * step * CORES

                @pl.when(sent)
                def _():
                    hop(chain, source, block, base + step, partner).wait_send()

        pltpu.make_async_copy(source, result.at[me], local_sem.at[op]).wait()
    for copy in simple:
        copy.wait()
    for copy in locals_:
        copy.wait()


def exchange(kinds, arrays, number):
    kinds = tuple(kinds)
    shapes = []
    for (name, axis), array in zip(kinds, arrays):
        size = lax.axis_size(axis)
        if name in ("gather", "chain"):
            shape = (size,) + array.shape
        elif name == "columns":
            shape = (size, array.shape[0], array.shape[1] // size)
        elif name == "scatter":
            shape = array.shape
        else:
            shape = (size // CORES,) + array.shape[1:]
        shapes.append(jax.ShapeDtypeStruct(shape, array.dtype))
    sems = [pltpu.SemaphoreType.DMA((count_copies(kind),)) for kind in kinds]
    return pl.pallas_call(
        functools.partial(exchange_kernel, kinds),
        out_shape=shapes,
        in_specs=[pl.BlockSpec(memory_space=pl.ANY)] * len(kinds),
        out_specs=[pl.BlockSpec(memory_space=pl.ANY)] * len(kinds),
        scratch_shapes=[pltpu.SemaphoreType.DMA((len(kinds),))] + sems + sems,
        compiler_params=pltpu.CompilerParams(collective_id=number, has_side_effects=True),
        name="exchange",
    )(*arrays)


def swapped(block, axis, bit):
    count = lax.axis_size(axis)
    route = []
    for low in range(count):
        high = low | 1 << bit
        if high != low and high < count:
            route += [(low, high), (high, low)]
    return lax.ppermute(block, axis, route)


def layer_norm(values, gain):
    center = values - jnp.mean(values, axis=-1, keepdims=True)
    spread = jnp.mean(center * center, axis=-1, keepdims=True)
    return center * lax.rsqrt(spread + 1e-05) * gain


def attend_block(block_queries, keys, values, valid, scale, layout):
    scores = (
        jnp.einsum(
            "thd," + layout + "->htk", block_queries, keys, preferred_element_type=jnp.float32
        )
        * scale
    )
    scores = jnp.where(valid[None, None, :], scores, -1e30)
    top = jnp.max(scores, axis=-1, keepdims=True)
    weights = jnp.exp(scores - top)
    probs = (weights / jnp.sum(weights, axis=-1, keepdims=True)).astype(jnp.bfloat16)
    return jnp.einsum("htk," + layout + "->thd", probs, values, preferred_element_type=jnp.float32)


def local(
    image,
    ln_gain,
    fc1_weight,
    fc2_weight,
    projector_weight,
    kv_weight,
    text,
    q_weight,
    o_weight,
    tile_count,
    text_start,
):
    inputs = image[0].astype(jnp.float32)
    group_count = lax.axis_size("mp")
    normed = layer_norm(inputs, ln_gain).astype(jnp.bfloat16)
    up, down, all_normed = exchange(
        (("chain", "mp"), ("chain", "mp"), ("gather", "dp")), (fc1_weight.T, fc2_weight, normed), 0
    )
    up = up.reshape(-1, up.shape[-1])
    down = down.reshape(-1, down.shape[-1])
    all_normed = all_normed.reshape(-1, all_normed.shape[-1])
    hidden = jax.nn.gelu(
        lax.dot_general(
            all_normed, up, (((1,), (1,)), ((), ())), preferred_element_type=jnp.float32
        ),
        approximate=False,
    ).astype(jnp.bfloat16)
    branch = jnp.dot(hidden, down, preferred_element_type=jnp.float32).astype(jnp.bfloat16)
    branch = branch.reshape((lax.axis_size("dp"),) + inputs.shape)

    kv_count = kv_weight.shape[1]
    devices_per_kv = group_count // kv_count
    kv_columns = kv_count * 2 * HEAD_DIM
    flat_kv = kv_weight.reshape(kv_weight.shape[0], kv_columns)
    row_count = projector_weight.shape[0] // lax.axis_size("dp")
    rows = lax.dynamic_slice_in_dim(
        projector_weight, lax.axis_index("dp") * row_count, row_count, axis=0
    )
    folded = jnp.dot(rows, flat_kv, preferred_element_type=jnp.float32).astype(jnp.bfloat16)
    terms, folded = exchange((("scatter", "dp"), ("columns", "mp")), (branch, folded), 1)
    encoded = (inputs + jnp.sum(terms.astype(jnp.float32), axis=0)).astype(jnp.bfloat16)
    folded = jnp.sum(folded.astype(jnp.float32), axis=0).astype(jnp.bfloat16)
    for bit_index in range(devices_per_kv.bit_length() - 1):
        partner = swapped(folded, "mp", bit_index)
        is_lower = lax.axis_index("mp") // (1 << bit_index) % 2 == 0
        folded = jnp.where(
            is_lower, jnp.concatenate([folded, partner], 1), jnp.concatenate([partner, folded], 1)
        )
    all_encoded, folded = exchange((("chain", "mp"), ("gather", "dp")), (encoded, folded), 2)
    all_encoded = all_encoded.reshape(-1, all_encoded.shape[-1])
    folded = folded.reshape(-1, folded.shape[-1])
    image_rows = all_encoded.shape[0]
    portion = jnp.einsum("rc,kr->ck", folded, all_encoded, preferred_element_type=jnp.float32)
    keys = portion[:HEAD_DIM]
    key_scale = lax.rsqrt(jnp.mean(keys * keys, axis=0, keepdims=True) + 1e-06)
    keys = (keys * key_scale).astype(jnp.bfloat16)
    values = portion[HEAD_DIM:].astype(jnp.bfloat16)
    layout = "dk"
    text_rows = text.shape[1]
    local_heads = q_weight.shape[1] // HEAD_DIM
    queries = jnp.dot(text[0], q_weight, preferred_element_type=jnp.float32).astype(jnp.bfloat16)
    queries = queries.reshape(text_rows, local_heads, HEAD_DIM)
    valid = jnp.arange(image_rows, dtype=jnp.int32) // TILE_TOK < tile_count[0]
    scale = 1.0 / HEAD_DIM**0.5
    block_rows = min(text_rows, 256)
    blocks = queries.reshape(text_rows // block_rows, block_rows, local_heads, HEAD_DIM)
    attended_heads = lax.map(
        lambda block_queries: attend_block(block_queries, keys, values, valid, scale, layout),
        blocks,
    )
    attended_heads = attended_heads.reshape(text_rows, local_heads * HEAD_DIM)
    row_mask = (jnp.arange(text_rows, dtype=jnp.int32) >= text_start[0]).astype(jnp.float32)
    heads_out = (attended_heads * row_mask[:, None]).astype(jnp.bfloat16)
    out = jnp.dot(heads_out, o_weight, preferred_element_type=jnp.float32).astype(jnp.bfloat16)
    out = out.reshape(group_count, text_rows // group_count, out.shape[-1])
    (theirs,) = exchange((("partner", "mp"),), (out,), 3)
    chip_out = out.reshape((group_count // CORES, CORES) + out.shape[1:])
    mine = lax.dynamic_index_in_dim(
        chip_out, lax.axis_index("mp") % CORES, axis=1, keepdims=False
    )
    paired = (mine.astype(jnp.float32) + theirs.astype(jnp.float32)).astype(jnp.bfloat16)
    (terms,) = exchange((("stride", "mp"),), (paired,), 4)
    summed_out = jnp.sum(terms.astype(jnp.float32), axis=0).astype(jnp.bfloat16)
    return summed_out[None]


def solution(mesh):
    return jax.shard_map(
        local,
        mesh=mesh,
        in_specs=(
            P("dp", "mp", None),
            P(),
            P(None, ("dp", "mp")),
            P(("dp", "mp"), None),
            P(None, "mp"),
            P("mp", None, None, None),
            P("dp", None, None),
            P(None, "mp"),
            P("mp", None),
            P("dp"),
            P("dp"),
        ),
        out_specs=P("dp", "mp", None),
        check_vma=False,
    )
```
